32 devices in a mesh: expert: 2 (over y), dp: 4 (over x, core), shard: 4 (over z).
Axes of the slice: x: 2, y: 2, z: 4, core: 2. Of those that a mesh axis runs over, the one named last changes fastest.
Arguments:
- grad_partials: bfloat16 [4, 2, 4096, 1536], P('dp', 'expert', 'shard'), may hold values from -120 to 120
- momentum: float32 [2, 4, 1024, 1536], P('expert', 'shard', 'dp'), may hold values from -3 to 3
- q_factor: float32 [1536, 2, 384], P(('dp', 'shard'), 'expert'), may hold values from -0.15625 to 0.15625
Outputs:
- next_momentum: float32 [2, 4, 1024, 1536], P('expert', 'shard', 'dp')
- next_factor: float32 [1536, 2, 384], P(('dp', 'shard'), 'expert')
- weight_update: bfloat16 [2, 4096, 1536], P('expert', 'shard')
The draws below stay inside these ranges and needn't reach their ends.
All inputs are finite; a program needn't handle non-finite values.
Results may differ from the reference program's by a relative error of at most 0.015.
Values may be sent and summed in bfloat16 or wider, within the bound.
A program may use at most 64 MiB of HBM per device.

```python
import math
import jax
import jax.numpy as jnp
from jax import lax

D = 4096
FF = 1536
R = 384
EXPERTS = 2
SHARD_ROWS = 1024
N_DP = 4
N_SHARD = 4


def draw_grad_partials(key, part):
    subkeys = jax.random.split(key, 3)
    log_span = math.log(10.0)
    row_scale = jnp.exp(jax.random.uniform(subkeys[0], (1, EXPERTS, D, 1), jnp.float32, 0.0, log_span))
    column_scale = jnp.exp(jax.random.uniform(subkeys[1], (1, EXPERTS, 1, FF), jnp.float32, 0.0, log_span))
    expert_place = jnp.arange(EXPERTS, dtype=jnp.float32).reshape(1, EXPERTS, 1, 1) / max(EXPERTS - 1, 1)
    row_place = jnp.arange(D, dtype=jnp.float32).reshape(1, 1, D, 1) / (D - 1)
    growth = jnp.exp(math.log(3.0) * 0.5 * (expert_place + row_place))
    entries = jnp.clip(jax.random.normal(subkeys[2], (N_DP, EXPERTS, D, FF), jnp.float32), -4.0, 4.0)
    return (0.1 * entries * row_scale * column_scale * growth).astype(jnp.bfloat16)


def shard_levels(key, extent, shards, smallest, high):
    def one(position, shards_of):
        draws = jax.random.uniform(jax.random.fold_in(jax.random.fold_in(key, 6), position), (shards_of,), jnp.float32, smallest / len(shards), high / len(shards))
        return jnp.repeat(jnp.exp(draws), extent[position] // shards_of).reshape((-1,) + (1,) * (len(extent) - position - 1))

    level = one(*shards[0])
    for cut in shards[1:]:
        level = level * one(*cut)
    return level


def centred(rng, extent, width, bound, shards=(), held_as=jnp.bfloat16):
    values = jax.random.normal(rng, extent, jnp.float32) * width
    if len(shards) > 0:
        values = shard_levels(rng, extent, shards, -0.22, 0.18) * values
    return jnp.clip(values, min=-bound, max=bound).astype(held_as)


def setup_inputs(seed: int = 0) -> dict:
    key_list = jax.random.split(jax.random.key(seed), 4)
    return {
        "grad_partials": draw_grad_partials(jax.random.fold_in(key_list[3], 71), 0),
        "momentum": centred(key_list[1], (EXPERTS, N_SHARD, SHARD_ROWS, FF), 0.5, 3.0, ((0, 2), (1, 4), (2, 4)), jnp.float32),
        "q_factor": centred(key_list[2], (FF, EXPERTS, R), FF ** -0.5, 0.15625, ((0, 16), (1, 2)), jnp.float32),
    }


clip_rms = 0.5
keep_share = 0.95
highest = lax.Precision.HIGHEST

def reference(grad_partials, momentum, q_factor):
    gradient = grad_partials[0].astype(jnp.float32)
    for replica in range(1, N_DP):
        gradient = gradient + grad_partials[replica].astype(jnp.float32)
    square_sum = jnp.sum(gradient * gradient)
    clip_scale = clip_rms / jnp.sqrt(square_sum / gradient.size + 1e-06)
    experts = gradient.shape[0]
    buffer = momentum.reshape(experts, D, FF) + clip_scale * gradient
    unit_scale = math.sqrt(D * FF / R)

    def per_expert(operands):
        buffer_one, factor_one = operands
        projected = jnp.dot(buffer_one, factor_one, precision=highest)
        gram_matrix = jnp.dot(projected.T, projected, precision=highest)
        triangle = jnp.linalg.cholesky(gram_matrix)
        ortho_basis = jax.scipy.linalg.solve_triangular(triangle, projected.T, lower=True).T
        right_factor = jnp.dot(buffer_one.T, ortho_basis, precision=highest)
        inverse = lax.rsqrt(lax.optimization_barrier(jnp.sum(right_factor * right_factor, axis=0)) + 1e-06)
        next_factor = right_factor * inverse
        correction = jnp.dot(ortho_basis, right_factor.T, precision=highest)
        direction = jnp.dot(ortho_basis * inverse, right_factor.T, precision=highest)
        next_momentum = buffer_one - (1.0 - keep_share) * correction
        weight_update = (unit_scale * direction).astype(jnp.bfloat16)
        return (next_momentum, next_factor, weight_update)
    next_momentum, next_factor, weight_update = lax.map(per_expert, (buffer, jnp.swapaxes(q_factor, 0, 1)))
    return (next_momentum.reshape(experts, N_SHARD, D // N_SHARD, FF), jnp.swapaxes(next_factor, 0, 1), weight_update)
```

```python
import functools
import math

import jax
import jax.numpy as jnp
from jax import lax
from jax.experimental import pallas as pl
from jax.experimental.pallas import tpu as pltpu
from jax.sharding import PartitionSpec as P

clip_rms = 0.5
keep_share = 0.95
highest = lax.Precision.HIGHEST
f32 = jnp.float32
bf16 = jnp.bfloat16


def split(a):
    hi = a.astype(bf16)
    return hi, (a - hi.astype(f32)).astype(bf16)


def contract(a, b, da, db):
    return lax.dot_general(a, b, (((da,), (db,)), ((), ())), preferred_element_type=f32)


def exact(a, b, da, db):
    return lax.dot_general(
        a, b, (((da,), (db,)), ((), ())), precision=highest, preferred_element_type=f32
    )


def inverse_factor(block):
    width = block.shape[0]
    panels = width // 8
    sub = lax.broadcasted_iota(jnp.int32, (8, width), 0)
    lane = lax.broadcasted_iota(jnp.int32, (8, width), 1)
    a = [block[8 * p : 8 * p + 8, :] for p in range(panels)]
    x = [jnp.where(lane == sub + 8 * p, 1.0, 0.0).astype(f32) for p in range(panels)]
    for j in range(width):
        p, r = divmod(j, 8)
        arow = a[p][r : r + 1, :]
        xrow = x[p][r : r + 1, :]
        scale = 1.0 / arow[:, j : j + 1]
        arow = arow * scale
        xrow = xrow * scale
        for q in range(p if r < 7 else p + 1, panels):
            col = a[q][:, j : j + 1]
            if q == p:
                col = jnp.where(sub[:, :1] > r, col, 0.0)
            a[q] = a[q] - col * arow
            x[q] = x[q] - col * xrow
        if r == 7:
            diag = jnp.sum(jnp.where(lane == sub + 8 * p, a[p], 0.0), axis=1, keepdims=True)
            x[p] = x[p] * lax.rsqrt(diag)
    return jnp.concatenate(x, axis=0)


def inverse_triangle(gram_ref, w_ref):
    rank = gram_ref.shape[0]
    size = 128 if rank % 128 == 0 else rank
    count = rank // size
    s = {
        (i, k): gram_ref[i * size : (i + 1) * size, k * size : (k + 1) * size]
        for i in range(count)
        for k in range(i + 1)
    }
    low = {}
    w = {}
    w_ref[...] = jnp.zeros_like(w_ref)
    for k in range(count):
        w[k, k] = inverse_factor(s[k, k])
        for i in range(k + 1, count):
            low[i, k] = exact(s[i, k], w[k, k], 1, 1)
        for i in range(k + 1, count):
            for m in range(k + 1, i + 1):
                s[i, m] = s[i, m] - exact(low[i, k], low[m, k], 1, 1)
        for m in range(k):
            total = exact(low[k, m], w[m, m], 1, 0)
            for t in range(m + 1, k):
                total = total + exact(low[k, t], w[t, m], 1, 0)
            w[k, m] = -exact(w[k, k], total, 1, 0)
        for m in range(k + 1):
            w_ref[k * size : (k + 1) * size, m * size : (m + 1) * size] = w[k, m]


def finish_kernel(unit_scale, q_ref, m_ref, rows_ref, buf_ref, mine_ref, nm_ref, right_ref, inv_ref, wu_ref, gram, w):
    qv = q_ref[...]
    m_hi, m_lo = split(m_ref[...])
    gram[...] = contract(qv, m_hi, 0, 0) + contract(qv, m_lo, 0, 0)
    inverse_triangle(gram, w)
    w_hi, w_lo = split(w[...])
    right = contract(m_hi, w_hi, 1, 1) + contract(m_hi, w_lo, 1, 1) + contract(m_lo, w_hi, 1, 1)
    right_ref[...] = right
    inverse = lax.rsqrt(jnp.sum(right * right, axis=0, keepdims=True) + 1e-06)
    inv_ref[...] = inverse
    right_b = right.astype(bf16)
    mine_hi, mine_lo = split(mine_ref[...])
    basis = contract(mine_hi, w_hi, 1, 1) + contract(mine_hi, w_lo, 1, 1) + contract(mine_lo, w_hi, 1, 1)
    nm_ref[...] = buf_ref[...] - (1.0 - keep_share) * contract(basis.astype(bf16), right_b, 1, 1)
    rows = rows_ref[...]
    every = contract(rows, w_hi, 1, 1) + contract(rows, w_lo, 1, 1)
    scaled = (every * (unit_scale * inverse)).astype(bf16)
    wu_ref[...] = contract(scaled, right_b, 1, 1).astype(bf16)


def finish(unit_scale, q, m, rows, buf, mine):
    hidden, rank = m.shape
    whole = pl.BlockSpec(memory_space=pltpu.VMEM)
    return pl.pallas_call(
        functools.partial(finish_kernel, unit_scale),
        out_shape=(
            jax.ShapeDtypeStruct(buf.shape, f32),
            jax.ShapeDtypeStruct((hidden, rank), f32),
            jax.ShapeDtypeStruct((1, rank), f32),
            jax.ShapeDtypeStruct((rows.shape[0], hidden), bf16),
        ),
        in_specs=[whole] * 5,
        out_specs=(whole,) * 4,
        scratch_shapes=[pltpu.VMEM((rank, rank), f32), pltpu.VMEM((rank, rank), f32)],
        compiler_params=pltpu.CompilerParams(vmem_limit_bytes=56 * 1024 * 1024),
    )(q, m, rows, buf, mine)


def shards(grad_partials, momentum, q_factor):
    partial_value = grad_partials[0]
    gradient = lax.psum_scatter(partial_value, "dp", scatter_dimension=1, tiled=True).astype(f32)
    momentum_rows = momentum[:, 0]
    experts, local_rows, hidden_width = gradient.shape
    factor_count, _, rank_width = q_factor.shape
    total_rows = local_rows * lax.axis_size("dp") * lax.axis_size("shard")
    entries = float(experts * lax.axis_size("expert") * total_rows * hidden_width)
    square_sum = lax.psum(jnp.sum(gradient * gradient), ("expert", "dp", "shard"))
    clip_scale = clip_rms / jnp.sqrt(square_sum / entries + 1e-06)
    buffer = (momentum_rows + clip_scale * gradient)[0]
    q_all = lax.all_gather(q_factor.astype(bf16)[:, 0], ("dp", "shard"), axis=0, tiled=True)
    projected = exact(buffer, q_all.astype(f32), 1, 0)
    moment = lax.psum(exact(buffer, projected, 0, 0), ("dp", "shard"))
    rows = lax.all_gather(projected.astype(bf16), "dp", axis=0, tiled=True)
    unit_scale = math.sqrt(total_rows * hidden_width / rank_width)
    next_momentum, right, inverse, update = finish(unit_scale, q_all, moment, rows, buffer, projected)
    offset = (
        lax.axis_index("dp") * lax.axis_size("shard") + lax.axis_index("shard")
    ) * factor_count
    next_factor = lax.dynamic_slice_in_dim(right, offset, factor_count, 0) * inverse
    return (next_momentum[None, None], next_factor[:, None], update[None])


def solution(mesh):
    placed = (
        P("dp", "expert", "shard", None),
        P("expert", "shard", "dp", None),
        P(("dp", "shard"), "expert", None),
    )
    return jax.shard_map(
        shards,
        mesh=mesh,
        in_specs=placed,
        out_specs=(
            P("expert", "shard", "dp", None),
            P(("dp", "shard"), "expert", None),
            P("expert", "shard", None),
        ),
        check_vma=False,
    )
```
